32 devices in a mesh: rep: 2 (over z, core), dp: 16 (over x, y).
Axes of the slice: x: 4, y: 4, z: 1, core: 2. Of those that a mesh axis runs over, the one named last changes fastest.
The devices are a block of a 4x4x8 slice.
Arguments:
- a: bfloat16 [32, 4, 4096, 512], P(('rep', 'dp')), parts along dimension 0
- g: bfloat16 [32, 4, 4096, 1792], P(('rep', 'dp')), parts along dimension 0
Outputs:
- output: bfloat16 [8, 512, 1792], P('rep'), parts along dimension 0
There are 2 independent parts. The reference program is written for one: setup_inputs(seed, part) draws one part's arguments, and reference() takes and returns one part's arrays. A program takes and returns all parts, laid end to end along the dimension named above; each array names one.
All inputs are finite; a program needn't handle non-finite values.
Results may differ from the reference program's by a relative error of at most 0.012.
Values are sent between devices in bfloat16 or wider.
A program may use at most 768 MiB of HBM per device.

```python
import jax
import jax.numpy as jnp
from jax import lax

DEVICES = 16
MATRICES = 4
TOKENS = 4096
D = 512
FF = 1792


def setup_inputs(seed: int = 0, part: int = 0) -> dict:
    ka, kg, ks = (jax.random.fold_in(k, part) for k in jax.random.split(jax.random.key(seed), 3))
    size = 2.0 ** jax.random.uniform(ks, (DEVICES, MATRICES, 1, 1), jnp.float32, -1.0, 1.0)
    a = jax.random.normal(ka, (DEVICES, MATRICES, TOKENS, D), jnp.float32)
    g = size * jax.random.normal(kg, (DEVICES, MATRICES, TOKENS, FF), jnp.float32) * (DEVICES * TOKENS) ** -0.5
    return {"a": a.astype(jnp.bfloat16), "g": g.astype(jnp.bfloat16)}


def reference(a, g):
    def take(so_far, one):
        return so_far + jnp.einsum("ntd,ntf->ndf", *one, preferred_element_type=jnp.float32), None

    return lax.scan(take, jnp.zeros((MATRICES, D, FF), jnp.float32), (a, g))[0].astype(jnp.bfloat16)
```

```python
import functools
import math

import jax
import jax.numpy as jnp
from jax import lax
from jax.experimental import pallas as pl
from jax.experimental.pallas import tpu as pltpu
from jax.sharding import PartitionSpec as P

MESH = pl.DeviceIdType.MESH
COLS = 256
LAGS = (3, 6, 9, 12, 15)
AG_LAGS = (2, 4)
RING = 8


def kernel(side, a_hbm, g_hbm, out, abuf, gbuf, acc, sb, r1, r2, acc2, sb2, r3, r4,
           asem, gsem, send, s1, s2, s3, s4, s5, s6, s7, s8):
    mats, _, rows = a_hbm.shape
    per = g_hbm.shape[2] // COLS
    units = mats * per
    slots = gbuf.shape[0]
    quarter = rows // side
    half = quarter // 2
    piece = quarter // side
    bit = piece // 2

    me = lax.axis_index("dp")
    x, y = me // side, me % side

    def place(u):
        f = u % 2
        s1_, s2_ = f + (1 - f) * side, f * side + (1 - f)
        p1, p2 = x * (1 - f) + y * f, y * (1 - f) + x * f

        def nbr(p, s, d):
            return me + ((p + d) % side - p) * s

        return ((p1, nbr(p1, s1_, 1), nbr(p1, s1_, side - 1)),
                (p2, nbr(p2, s2_, 1), nbr(p2, s2_, side - 1)))

    def put(src, dst, u, sem, to):
        pltpu.make_async_remote_copy(
            src_ref=src, dst_ref=dst, send_sem=send.at[u], recv_sem=sem.at[u],
            device_id={"dp": to}, device_id_type=MESH).start()

    def got(ref, u, sem):
        pltpu.make_async_remote_copy(
            src_ref=ref, dst_ref=ref, send_sem=send.at[u], recv_sem=sem.at[u],
            device_id={"dp": me}, device_id_type=MESH).wait_recv()

    def load_a(n):
        return pltpu.make_async_copy(a_hbm.at[n], abuf.at[n % 2], asem.at[n % 2])

    def load_g(u):
        return pltpu.make_async_copy(
            g_hbm.at[u // per, :, pl.ds(pl.multiple_of(u % per * COLS, COLS), COLS)],
            gbuf.at[u % slots], gsem.at[u % slots])

    def cut(start, size):
        return pl.ds(pl.multiple_of(start, bit), size)

    def cols(u):
        return pl.ds(pl.multiple_of(u % per * COLS, COLS), COLS)

    def scatter_first(u, p, plus, minus, src, near, far, big, small):
        (near_buf, near_sem), (far_buf, far_sem) = near, far
        opp, up, down = (p + 2) % side, (p + 1) % side, (p + side - 1) % side
        put(src.at[u, cut(opp * big, small)], far_buf.at[u, 0], u, far_sem, plus)
        put(src.at[u, cut(opp * big + small, small)], far_buf.at[u, 1], u, far_sem, minus)
        put(src.at[u, cut(up * big + small, small)], near_buf.at[u, 0, pl.ds(small, small)], u, near_sem, plus)
        put(src.at[u, cut(down * big, small)], near_buf.at[u, 1, pl.ds(0, small)], u, near_sem, minus)

    def scatter_second(u, p, plus, minus, total, src, near, far, big, small):
        (near_buf, near_sem), (far_buf, far_sem) = near, far
        up, down = (p + 1) % side, (p + side - 1) % side
        got(far_buf.at[u], u, far_sem)
        k = u % RING
        src[u, cut(up * big, small)] = (
            total[k, cut(up * big, small)] + far_buf[u, 0].astype(jnp.float32)).astype(src.dtype)
        src[u, cut(down * big + small, small)] = (
            total[k, cut(down * big + small, small)] + far_buf[u, 1].astype(jnp.float32)).astype(src.dtype)
        put(src.at[u, cut(up * big, small)], near_buf.at[u, 0, pl.ds(0, small)], u, near_sem, plus)
        put(src.at[u, cut(down * big + small, small)], near_buf.at[u, 1, pl.ds(small, small)], u, near_sem, minus)

    def compute(u):
        n = u // per

        @pl.when(u % per == 0)
        def _():
            load_a(n).wait()

            @pl.when(n + 1 < mats)
            def _():
                load_a(n + 1).start()

        load_g(u).wait()
        res = lax.dot_general(abuf[n % 2], gbuf[u % slots], (((0,), (0,)), ((), ())),
                              preferred_element_type=jnp.float32)
        acc[u % RING] = res
        sb[u] = res.astype(sb.dtype)

        @pl.when(u + slots < units)
        def _():
            load_g(u + slots).start()

        (p, plus, minus), _ = place(u)
        scatter_first(u, p, plus, minus, sb, (r2, s2), (r1, s1), quarter, half)

    def step1(u):
        (p, plus, minus), _ = place(u)
        scatter_second(u, p, plus, minus, acc, sb, (r2, s2), (r1, s1), quarter, half)

    def step2(u):
        (p1, _, _), (p, plus, minus) = place(u)
        got(r2.at[u], u, s2)
        k = u % RING
        t = acc[k, cut(p1 * quarter, quarter)] + r2[u, 0].astype(jnp.float32) + r2[u, 1].astype(jnp.float32)
        acc2[k] = t
        sb2[u] = t.astype(sb2.dtype)
        scatter_first(u, p, plus, minus, sb2, (r4, s4), (r3, s3), piece, bit)

    def step3(u):
        _, (p, plus, minus) = place(u)
        scatter_second(u, p, plus, minus, acc2, sb2, (r4, s4), (r3, s3), piece, bit)

    def mine(u, start, size):
        return out.at[u // per, cut(start, size), cols(u)]

    def step4(u):
        (p1, _, _), (p, plus, minus) = place(u)
        got(r4.at[u], u, s4)
        t = acc2[u % RING, cut(p * piece, piece)] + r4[u, 0].astype(jnp.float32) + r4[u, 1].astype(jnp.float32)
        at = p1 * quarter + p * piece
        out[u // per, cut(at, piece), cols(u)] = t.astype(out.dtype)
        put(mine(u, at, piece), mine(u, at, piece), u, s5, plus)
        put(mine(u, at, piece), mine(u, at, piece), u, s5, minus)

    def gather1(u):
        (p1, _, _), (p, plus, minus) = place(u)
        got(r2.at[u, 0, pl.ds(0, 2 * piece)], u, s5)
        at = p1 * quarter
        low, high = at + (p + side - 1) % side * piece, at + (p + 1) % side * piece + bit
        put(mine(u, low, bit), mine(u, low, bit), u, s6, plus)
        put(mine(u, high, bit), mine(u, high, bit), u, s6, minus)

    def gather2(u):
        (p, plus, minus), _ = place(u)
        got(r2.at[u, 0, pl.ds(0, piece)], u, s6)
        at = p * quarter
        put(mine(u, at, quarter), mine(u, at, quarter), u, s7, plus)
        put(mine(u, at, quarter), mine(u, at, quarter), u, s7, minus)

    def gather3(u):
        (p, plus, minus), _ = place(u)
        got(r2.at[u], u, s7)
        low, high = (p + side - 1) % side * quarter, (p + 1) % side * quarter + half
        put(mine(u, low, half), mine(u, low, half), u, s8, plus)
        put(mine(u, high, half), mine(u, high, half), u, s8, minus)

    def gather4(u):
        got(r2.at[u, 0], u, s8)

    def staged(t, lag, f):
        @pl.when((t >= lag) & (t < units + lag))
        def _():
            f(t - lag)

    load_a(0).start()
    for u in range(slots):
        load_g(u).start()

    barrier = pltpu.get_barrier_semaphore()
    for place_ in place(0):
        for to in place_[1:]:
            pl.semaphore_signal(barrier, inc=1, device_id={"dp": to}, device_id_type=MESH)
    pl.semaphore_wait(barrier, 4)

    @pl.loop(0, units + LAGS[-1])
    def _(t):
        staged(t, 0, compute)
        for lag, f in zip(LAGS, (step1, step2, step3, step4, gather1)):
            staged(t, lag, f)

    @pl.loop(0, units + AG_LAGS[-1])
    def _(t):
        staged(t, 0, gather2)
        for lag, f in zip(AG_LAGS, (gather3, gather4)):
            staged(t, lag, f)

    @pl.loop(0, units)
    def _(u):
        for ref, times in ((r2.at[u, 0], 6), (r4.at[u, 0], 6)):
            for _ in range(times):
                pltpu.make_async_remote_copy(
                    src_ref=ref, dst_ref=ref, send_sem=send.at[u], recv_sem=s1.at[u],
                    device_id={"dp": me}, device_id_type=MESH).wait_send()


def solution(mesh):
    side = math.isqrt(mesh.shape["dp"])

    def body(a, g):
        a, g = a[0], g[0]
        mats, tokens, rows = a.shape
        width = g.shape[2]
        units = mats * (width // COLS)
        quarter = rows // side
        piece = quarter // side
        bf16, f32 = jnp.bfloat16, jnp.float32
        dma = pltpu.SemaphoreType.DMA
        slots = 3
        return pl.pallas_call(
            functools.partial(kernel, side),
            out_shape=jax.ShapeDtypeStruct((mats, rows, width), bf16),
            in_specs=[pl.BlockSpec(memory_space=pl.ANY)] * 2,
            out_specs=pl.BlockSpec(memory_space=pltpu.VMEM),
            scratch_shapes=[
                pltpu.VMEM((2, tokens, rows), bf16),
                pltpu.VMEM((slots, tokens, COLS), bf16),
                pltpu.VMEM((RING, rows, COLS), f32),
                pltpu.VMEM((units, rows, COLS), bf16),
                pltpu.VMEM((units, 2, quarter // 2, COLS), bf16),
                pltpu.VMEM((units, 2, quarter, COLS), bf16),
                pltpu.VMEM((RING, quarter, COLS), f32),
                pltpu.VMEM((units, quarter, COLS), bf16),
                pltpu.VMEM((units, 2, piece // 2, COLS), bf16),
                pltpu.VMEM((units, 2, piece, COLS), bf16),
                dma((2,)), dma((slots,)), dma((units,)),
            ] + [dma((units,))] * 8,
            compiler_params=pltpu.CompilerParams(
                collective_id=0, has_side_effects=True, vmem_limit_bytes=56 << 20),
        )(a, g)

    return jax.shard_map(
        body, mesh=mesh, in_specs=(P(("rep", "dp")), P(("rep", "dp"))),
        out_specs=P("rep"), check_vma=False)
```

```python
import functools
import math

import jax
import jax.numpy as jnp
from jax import lax
from jax.experimental import pallas as pl
from jax.experimental.pallas import tpu as pltpu
from jax.sharding import PartitionSpec as P

MESH = pl.DeviceIdType.MESH
COLS = 256
LAGS = (3,6,9,12,15,19,30,45)
RING = 8
SLOTS = 4
CHUNKS = 4


def kernel(side, a_hbm, g_hbm, out, abuf, gbuf, acc, sb, r1, r2, acc2, sb2, r3, r4,
           first_sem, asem, gsem, send, *sems):
    s1, s2, s3, s4, s5, s6, s7, s8 = sems
    mats, tokens, rows = a_hbm.shape
    per = g_hbm.shape[2] // COLS
    units = mats * per
    quarter = rows // side
    half = quarter // 2
    piece = quarter // side
    bit = piece // 2

    me = lax.axis_index("dp")
    x, y = lax.div(me, side), lax.rem(me, side)

    def axis(p, stride):
        at = [lax.rem(p + d, side) for d in range(side)]
        return at, me + (at[1] - p) * stride, me + (at[side - 1] - p) * stride

    axes = (axis(x, side), axis(y, 1))
    order = ((axes[0], axes[1]), (axes[1], axes[0]))

    def put(src, dst, u, sem, to):
        pltpu.make_async_remote_copy(
            src_ref=src, dst_ref=dst, send_sem=send.at[u], recv_sem=sem.at[u],
            device_id={"dp": to}, device_id_type=MESH).start()

    def got(ref, u, sem):
        pltpu.make_async_remote_copy(
            src_ref=ref, dst_ref=ref, send_sem=send.at[u], recv_sem=sem.at[u],
            device_id={"dp": me}, device_id_type=MESH).wait_recv()

    def load_a(n):
        return pltpu.make_async_copy(a_hbm.at[n], abuf.at[lax.rem(n, 2)], asem.at[lax.rem(n, 2)])

    def cols(u, n):
        return pl.ds(pl.multiple_of((u - n * per) * COLS, COLS), COLS)

    def load_g(u):
        n = lax.div(u, per)
        at = cols(u, n)
        slot = lax.rem(u, SLOTS)
        return pltpu.make_async_copy(g_hbm.at[n, :, at], gbuf.at[slot], gsem.at[slot])

    def load_first(c):
        at = pl.ds(c * (tokens // CHUNKS), tokens // CHUNKS)
        return (pltpu.make_async_copy(a_hbm.at[0, at], abuf.at[0, at], first_sem.at[2 * c]),
                pltpu.make_async_copy(g_hbm.at[0, at, pl.ds(0, COLS)], gbuf.at[0, at], first_sem.at[2 * c + 1]))

    def cut(start, size):
        return pl.ds(pl.multiple_of(start, bit), size)

    def f32(v):
        return v.astype(jnp.float32)

    def first_sends(u, axis, src, near, near_sem, far, far_sem, big, small):
        at, plus, minus = axis
        opp, up, down = at[2] * big, at[1] * big, at[side - 1] * big
        put(src.at[u, cut(opp, small)], far.at[u, 0], u, far_sem, plus)
        put(src.at[u, cut(opp + small, small)], far.at[u, 1], u, far_sem, minus)
        put(src.at[u, cut(up + small, small)], near.at[u, 0, pl.ds(small, small)], u, near_sem, plus)
        put(src.at[u, cut(down, small)], near.at[u, 1, pl.ds(0, small)], u, near_sem, minus)

    def second_sends(u, axis, total, src, near, near_sem, far, far_sem, big, small):
        at, plus, minus = axis
        up, down = cut(at[1] * big, small), cut(at[side - 1] * big + small, small)
        k = lax.rem(u, RING)
        got(far.at[u], u, far_sem)
        src[u, up] = (total[k, up] + f32(far[u, 0])).astype(src.dtype)
        src[u, down] = (total[k, down] + f32(far[u, 1])).astype(src.dtype)
        put(src.at[u, up], near.at[u, 0, pl.ds(0, small)], u, near_sem, plus)
        put(src.at[u, down], near.at[u, 1, pl.ds(small, small)], u, near_sem, minus)

    def dot(lhs, rhs):
        return lax.dot_general(lhs, rhs, (((0,), (0,)), ((), ())), preferred_element_type=jnp.float32)

    def first_unit():
        for c in range(CHUNKS):
            at = pl.ds(c * (tokens // CHUNKS), tokens // CHUNKS)
            for copy in load_first(c):
                copy.wait()
            res = dot(abuf[0, at], gbuf[0, at])
            if c:
                res = res + acc[0]
            acc[0] = res
        sb[0] = res.astype(sb.dtype)
        first_sends(0, order[0][0], sb, r2, s2, r1, s1, quarter, half)

    def compute(u, f):
        n = lax.div(u, per)
        slot = lax.rem(u, SLOTS)

        @pl.when(u + 2 < units)
        def _():
            load_g(u + 2).start()

        @pl.when((u == n * per + 1) & (n + 1 < mats))
        def _():
            load_a(n + 1).start()

        load_g(u).wait()

        @pl.when(u == n * per)
        def _():
            load_a(n).wait()

        res = dot(abuf[lax.rem(n, 2)], gbuf[slot])
        acc[lax.rem(u, RING)] = res
        sb[u] = res.astype(sb.dtype)
        first_sends(u, order[f][0], sb, r2, s2, r1, s1, quarter, half)

    def step1(u, f):
        second_sends(u, order[f][0], acc, sb, r2, s2, r1, s1, quarter, half)

    def step2(u, f):
        own = cut(order[f][0][0][0] * quarter, quarter)
        k = lax.rem(u, RING)
        got(r2.at[u], u, s2)
        t = acc[k, own] + f32(r2[u, 0]) + f32(r2[u, 1])
        acc2[k] = t
        sb2[u] = t.astype(sb2.dtype)
        first_sends(u, order[f][1], sb2, r4, s4, r3, s3, piece, bit)

    def step3(u, f):
        second_sends(u, order[f][1], acc2, sb2, r4, s4, r3, s3, piece, bit)

    def pass_on(u, start, size, sem, to):
        n = lax.div(u, per)
        ref = out.at[n, cut(start, size), cols(u, n)]
        put(ref, ref, u, sem, to)

    def step4(u, f):
        (at1, _, _), (at2, plus, minus) = order[f]
        got(r4.at[u], u, s4)
        t = acc2[lax.rem(u, RING), cut(at2[0] * piece, piece)] + f32(r4[u, 0]) + f32(r4[u, 1])
        at = at1[0] * quarter + at2[0] * piece
        n = lax.div(u, per)
        out[n, cut(at, piece), cols(u, n)] = t.astype(out.dtype)
        pass_on(u, at, piece, s5, plus)
        pass_on(u, at, piece, s5, minus)

    def gather1(u, f):
        (at1, _, _), (at2, plus, minus) = order[f]
        got(r2.at[u, 0, pl.ds(0, 2 * piece)], u, s5)
        pass_on(u, at1[0] * quarter + at2[side - 1] * piece, bit, s6, plus)
        pass_on(u, at1[0] * quarter + at2[1] * piece + bit, bit, s6, minus)

    def gather2(u, f):
        at, plus, minus = order[f][0]
        got(r2.at[u, 0, pl.ds(0, piece)], u, s6)
        pass_on(u, at[0] * quarter, quarter, s7, plus)
        pass_on(u, at[0] * quarter, quarter, s7, minus)

    def gather3(u, f):
        at, plus, minus = order[f][0]
        got(r2.at[u], u, s7)
        pass_on(u, at[side - 1] * quarter, half, s8, plus)
        pass_on(u, at[1] * quarter + half, half, s8, minus)

    def gather4(u, f):
        got(r2.at[u, 0], u, s8)
        for ref, times in ((r2.at[u], 3), (r4.at[u], 3)):
            for _ in range(times):
                pltpu.make_async_remote_copy(
                    src_ref=ref, dst_ref=ref, send_sem=send.at[u], recv_sem=s1.at[u],
                    device_id={"dp": me}, device_id_type=MESH).wait_send()

    for c in range(CHUNKS):
        for copy in load_first(c):
            copy.start()
    load_g(1).start()

    barrier = pltpu.get_barrier_semaphore()
    for _, plus, minus in axes:
        for to in (plus, minus):
            pl.semaphore_signal(barrier, inc=1, device_id={"dp": to}, device_id_type=MESH)
    pl.semaphore_wait(barrier, 4)

    load_g(2).start()
    first_unit()
    stages = (compute, step1, step2, step3, step4, gather1, gather2, gather3, gather4)
    steps = units + LAGS[-1]

    @pl.loop(0, (steps + 1) // 2)
    def _(v):
        for k in range(2):
            for lag, stage in zip((0,) + LAGS, stages):
                u = 2 * v + (k - lag)

                @pl.when((u >= (1 if stage is compute else 0)) & (u < units))
                def _():
                    stage(u, (k - lag) % 2)


def solution(mesh):
    side = math.isqrt(mesh.shape["dp"])

    def body(a, g):
        a, g = a[0], g[0]
        mats, tokens, rows = a.shape
        width = g.shape[2]
        per = width // COLS
        units = mats * per
        quarter = rows // side
        piece = quarter // side
        bf16, f32 = jnp.bfloat16, jnp.float32
        dma = pltpu.SemaphoreType.DMA
        return pl.pallas_call(
            functools.partial(kernel, side),
            out_shape=pltpu.VMEM((mats, rows, width), bf16),
            in_specs=[pl.BlockSpec(memory_space=pl.ANY)] * 2,
            out_specs=pl.BlockSpec(memory_space=pltpu.VMEM),
            scratch_shapes=[
                pltpu.VMEM((2, tokens, rows), bf16),
                pltpu.VMEM((SLOTS, tokens, COLS), bf16),
                pltpu.VMEM((RING, rows, COLS), f32),
                pltpu.VMEM((units, rows, COLS), bf16),
                pltpu.VMEM((units, 2, quarter // 2, COLS), bf16),
                pltpu.VMEM((units, 2, quarter, COLS), bf16),
                pltpu.VMEM((RING, quarter, COLS), f32),
                pltpu.VMEM((units, quarter, COLS), bf16),
                pltpu.VMEM((units, 2, piece // 2, COLS), bf16),
                pltpu.VMEM((units, 2, piece, COLS), bf16),
                dma((2 * CHUNKS,)), dma((2,)), dma((SLOTS,)),
            ] + [dma((units,))] * 9,
            compiler_params=pltpu.CompilerParams(
                collective_id=0, has_side_effects=True, vmem_limit_bytes=42 << 20),
        )(a, g)

    return jax.shard_map(
        body, mesh=mesh, in_specs=(P(("rep", "dp")), P(("rep", "dp"))),
        out_specs=P("rep"), check_vma=False)
```
